8 devices in a mesh: dp: 2 (over y, z), sp: 4 (over x, core).
Axes of the slice: x: 2, y: 2, z: 1, core: 2. Of those that a mesh axis runs over, the one named last changes fastest.
Arguments:
- q: bfloat16 [64, 24, 128], P('dp'), parts along dimension 0
- k: bfloat16 [64, 4096, 8, 128], P('dp', 'sp'), parts along dimension 0
- v: bfloat16 [64, 4096, 8, 128], P('dp', 'sp'), parts along dimension 0
Outputs:
- q: bfloat16 [64, 24, 128], P('dp'), parts along dimension 0
There are 2 independent parts. The reference program is written for one: setup_inputs(seed, part) draws one part's arguments, and reference() takes and returns one part's arrays. A program takes and returns all parts, laid end to end along the dimension named above; each array names one.
All inputs are finite; a program needn't handle non-finite values.
Results may differ from the reference program's by a relative error of at most 0.012.
Values are sent between devices in bfloat16 or wider.
A program may use at most 2 GiB of HBM per device.

```python
import jax
import jax.numpy as jnp

BATCH = 32
CACHE = 4096
HEADS = 24
KV_HEADS = 8
HEAD = 128


def setup_inputs(seed: int = 0, part: int = 0) -> dict:
    kq, kk, kv = (jax.random.fold_in(k, part) for k in jax.random.split(jax.random.key(seed), 3))
    return {
        "q": (3 * jax.random.normal(kq, (BATCH, HEADS, HEAD), jnp.float32)).astype(jnp.bfloat16),
        "k": jax.random.normal(kk, (BATCH, CACHE, KV_HEADS, HEAD), jnp.float32).astype(jnp.bfloat16),
        "v": jax.random.normal(kv, (BATCH, CACHE, KV_HEADS, HEAD), jnp.float32).astype(jnp.bfloat16),
    }


def einsum(form, a, b):
    return jnp.einsum(form, a.astype(jnp.float32), b.astype(jnp.float32))


def reference(q, k, v):
    grouped = q.reshape(BATCH, KV_HEADS, -1, HEAD)
    scores = einsum("bgsd,bugd->bgsu", grouped, k) * HEAD**-0.5
    weights = jax.nn.softmax(scores, -1).astype(jnp.bfloat16)
    return einsum("bgsu,bugd->bgsd", weights, v).astype(jnp.bfloat16).reshape(BATCH, HEADS, HEAD)
```

```python
import functools
import math

import jax
import jax.numpy as jnp
from jax import lax
from jax.experimental import pallas as pl
from jax.experimental.pallas import tpu as pltpu
from jax.sharding import PartitionSpec as P

KEYS = 6
VALUES = 6
LAG = 2
CHUNKS = 4
MESH = pl.DeviceIdType.MESH


def kernel(n, groups, q_hbm, k_hbm, v_hbm, o_hbm, q_ref, kb, vb, s0, s1, p0, p1, m0, m1, stats, parts, out, q_sem, k_sem, v_sem, last_sem, o_sem, send, recv, stat_send, stat_recv):
    heads, head = q_ref.shape[1:]
    rows = kb.shape[1]
    half = rows // 2
    tiles = half // 128
    key_heads = groups[0]
    scale = head**-0.5 * math.log2(math.e)
    me = lax.axis_index("sp")
    size = parts.shape[0]
    s_bufs, p_bufs, m_bufs = (s0, s1), (p0, p1), (m0, m1)
    lane = lax.broadcasted_iota(jnp.int32, (heads, 128), 1)

    def peer(d):
        return {"sp": lax.rem(me + d, size)}

    def source(d):
        return lax.rem(me + size - d, size)

    def k_copy(i):
        slot = lax.rem(i, KEYS)
        return pltpu.make_async_copy(k_hbm.at[i], kb.at[slot], k_sem.at[slot])

    def v_copy(i):
        slot = lax.rem(i, VALUES)
        return pltpu.make_async_copy(v_hbm.at[i], vb.at[slot], v_sem.at[slot])

    def last_copy(c):
        slot, step = (n - 1) % VALUES, half // CHUNKS
        return [
            pltpu.make_async_copy(v_hbm.at[n - 1, pl.ds(h * half + c * step, step)], vb.at[slot, pl.ds(h * half + c * step, step)], last_sem.at[h, c])
            for h in range(2)
        ]

    def part_copy(d, first, count, late, slot):
        ref = parts.at[slot, pl.ds(first, count)]
        return pltpu.make_async_remote_copy(ref, ref, send.at[d - 1], recv.at[d - 1, late], device_id=peer(d), device_id_type=MESH)

    def stat_copy(d, slot):
        return pltpu.make_async_remote_copy(stats.at[slot], stats.at[slot], stat_send.at[d - 1], stat_recv.at[d - 1], device_id=peer(d), device_id_type=MESH)

    def scores(i, u):
        q = q_ref[i]
        none = jnp.zeros_like(q)
        both = jnp.concatenate([jnp.concatenate([q, none], 1), jnp.concatenate([none, q], 1)], 0)
        slot = lax.rem(i, KEYS)
        keys = jnp.concatenate([kb[slot, :half], kb[slot, half:]], 1)
        s = lax.dot_general(both, keys, (((1,), (1,)), ((), ())), preferred_element_type=jnp.float32)
        s = jnp.where(jnp.tile(own, (1, tiles)), s, -jnp.inf)
        s_bufs[u][...] = s
        high = functools.reduce(jnp.maximum, [s[:, j * 128 : (j + 1) * 128] for j in range(tiles)])
        m_bufs[u][...] = jnp.maximum(high[:heads], high[heads:])

    def weights(i, u):
        high = jnp.max(m_bufs[u][...], 1, keepdims=True)
        w = jnp.exp2((s_bufs[u][...] - jnp.concatenate([high, high], 0)) * scale)
        p_bufs[u][lax.rem(lax.div(i, 2), LAG // 2)] = w.astype(jnp.bfloat16)
        total = functools.reduce(jnp.add, [w[:, j * 128 : (j + 1) * 128] for j in range(tiles)])
        total = jnp.sum(total[:heads] + total[heads:], 1, keepdims=True)
        stats[me, 0] = jnp.where(lane == i, high, stats[me, 0])
        stats[me, 1] = jnp.where(lane == i, total, stats[me, 1])

    def seen(i, u, begin, end, cuts):
        slot = lax.rem(i, VALUES)
        w = p_bufs[u].at[lax.rem(lax.div(i, 2), LAG // 2)]
        step = (end - begin) // cuts
        o = None
        for c in range(cuts):
            b = begin + c * step
            values = jnp.concatenate([vb[slot, b : b + step], vb[slot, half + b : half + b + step]], 1)
            x = jnp.dot(w[:, b : b + step], values, preferred_element_type=jnp.float32)
            o = x if o is None else o + x
        return o[:heads, :head] + o[heads:, head:]

    def keep(i, o):
        parts[me, i] = o.astype(jnp.bfloat16)

    def share(first, count, late):
        for d in range(1, size):
            part_copy(d, first, count, late, me).start()

    q_copy = pltpu.make_async_copy(q_hbm, q_ref, q_sem)
    q_copy.start()
    for t in range(max(KEYS, VALUES + LAG)):
        if t < KEYS:
            k_copy(t).start(priority=1)
        if 0 <= t - LAG < VALUES:
            v_copy(t - LAG).start(priority=1)
    barrier = pltpu.get_barrier_semaphore()
    for d in range(1, size):
        pl.semaphore_signal(barrier, inc=1, device_id=peer(d), device_id_type=MESH)
    row = lax.broadcasted_iota(jnp.int32, (2 * heads, 128), 0)
    col = lax.broadcasted_iota(jnp.int32, (2 * heads, 128), 1)
    own = lax.rem(col, key_heads) == lax.div(lax.rem(row, heads), heads // key_heads)
    stats[me] = jnp.ones_like(stats[me])
    q_copy.wait()

    k_copy(0).wait()
    scores(0, 0)
    k_copy(1).wait()
    scores(1, 1)
    weights(0, 0)
    k_copy(KEYS).start(priority=1)
    k_copy(KEYS + 1).start(priority=1)

    def start_last():
        for c in range(CHUNKS):
            for copy in last_copy(c):
                copy.start(priority=1)

    def early(j, carry):
        for u in range(2):
            k_copy(2 * j + u).wait()
        for u in range(2):
            scores(2 * j + u, u)
            weights(2 * j + u - 1, 1 - u)
        for u in range(2):
            k_copy(2 * j + u + KEYS).start(priority=1)
        return carry

    lax.fori_loop(1, LAG // 2, early, 0)
    pl.semaphore_wait(barrier, size - 1)

    def step(j, carry):
        for u in range(2):
            k_copy(2 * j + u).wait()
            v_copy(2 * j + u - LAG).wait()
        for u in range(2):
            t = 2 * j + u
            keep(t - LAG, seen(t - LAG, u, 0, half, 2))
            scores(t, u)
            weights(t - 1, 1 - u)
        share(2 * j - LAG, 2, 0)
        for u in range(2):
            t = 2 * j + u

            @pl.when(t + KEYS < n)
            def _():
                k_copy(t + KEYS).start(priority=1)

            @pl.when(t - LAG + VALUES < n - 1)
            def _():
                v_copy(t - LAG + VALUES).start(priority=1)

            @pl.when(t - LAG + VALUES == n - 1)
            def _():
                start_last()

        return carry

    lax.fori_loop(LAG // 2, n // 2, step, 0)
    weights(n - 1, 1)
    for d in range(1, size):
        stat_copy(d, me).start()

    def late(j, carry):
        for u in range(2):
            i = 2 * j + u
            v_copy(i).wait()
            keep(i, seen(i, u, 0, half, 2))
        share(2 * j, 2, 0)
        return carry

    lax.fori_loop((n - LAG) // 2, n // 2 - 1, late, 0)
    v_copy(n - 2).wait()
    keep(n - 2, seen(n - 2, 0, 0, half, 2))
    share(n - 2, 1, 1)
    o = None
    for c in range(CHUNKS):
        for copy in last_copy(c):
            copy.wait()
        x = seen(n - 1, 1, c * (half // CHUNKS), (c + 1) * (half // CHUNKS), 2)
        o = x if o is None else o + x
    keep(n - 1, o)
    share(n - 1, 1, 1)

    for d in range(1, size):
        stat_copy(d, source(d)).wait_recv()
    highs = [stats[r, 0] for r in range(size)]
    high = functools.reduce(jnp.maximum, highs)
    factors = [jnp.exp2((h - high) * scale) for h in highs]
    total = functools.reduce(jnp.add, [f * stats[r, 1] for r, f in enumerate(factors)])
    factors = [f / total for f in factors]

    def together(i):
        terms = [parts[r, i].astype(jnp.float32) * f[:, i : i + 1] for r, f in enumerate(factors)]
        out[i] = functools.reduce(jnp.add, terms).astype(out.dtype)

    for d in range(1, size):
        part_copy(d, 0, n - 2, 0, source(d)).wait_recv()
    for i in range(n - 2):
        together(i)
    most = pltpu.make_async_copy(out.at[pl.ds(0, n - 2)], o_hbm.at[pl.ds(0, n - 2)], o_sem.at[0])
    most.start()
    for d in range(1, size):
        part_copy(d, n - 2, 2, 1, source(d)).wait_recv()
    for x in range(2):
        together(n - 2 + x)
    rest = pltpu.make_async_copy(out.at[pl.ds(n - 2, 2)], o_hbm.at[pl.ds(n - 2, 2)], o_sem.at[1])
    rest.start()
    for d in range(1, size):
        stat_copy(d, me).wait_send()
        part_copy(d, 0, n, 0, me).wait_send()
    most.wait()
    rest.wait()


def solution(mesh):
    size = mesh.shape["sp"]

    def step(q, k, v):
        n, heads, head = q.shape
        tokens, key_heads = k.shape[1:3]
        rows = tokens * key_heads
        half = rows // 2
        f32 = jnp.float32
        dma = pltpu.SemaphoreType.DMA
        return pl.pallas_call(
            functools.partial(kernel, n, (key_heads,)),
            out_shape=jax.ShapeDtypeStruct(q.shape, q.dtype),
            in_specs=[pl.BlockSpec(memory_space=pl.ANY)] * 3,
            out_specs=pl.BlockSpec(memory_space=pl.ANY),
            scratch_shapes=[
                pltpu.VMEM(q.shape, q.dtype),
                pltpu.VMEM((KEYS, rows, head), k.dtype),
                pltpu.VMEM((VALUES, rows, head), v.dtype),
                *[pltpu.VMEM((2 * heads, half), f32)] * 2,
                *[pltpu.VMEM((LAG // 2, 2 * heads, half), jnp.bfloat16)] * 2,
                *[pltpu.VMEM((heads, 128), f32)] * 2,
                pltpu.VMEM((size, 2, heads, 128), f32),
                pltpu.VMEM((size, n, heads, head), jnp.bfloat16),
                pltpu.VMEM(q.shape, q.dtype),
                dma,
                dma((KEYS,)),
                dma((VALUES,)),
                dma((2, CHUNKS)),
                dma((2,)),
                dma((size - 1,)),
                dma((size - 1, 2)),
                dma((size - 1,)),
                dma((size - 1,)),
            ],
            compiler_params=pltpu.CompilerParams(collective_id=0, has_side_effects=True, vmem_limit_bytes=60 * 2**20),
            name="attend",
        )(q, k.reshape(n, rows, head), v.reshape(n, rows, head))

    return jax.shard_map(
        step,
        mesh=mesh,
        in_specs=(P("dp", None, None), P("dp", "sp", None, None), P("dp", "sp", None, None)),
        out_specs=P("dp", None, None),
        check_vma=False,
    )
```

```python
import functools
import math

import jax
import jax.numpy as jnp
from jax import lax
from jax.experimental import pallas as pl
from jax.experimental.pallas import tpu as pltpu
from jax.sharding import PartitionSpec as P

KEYS = 8
VALUES = 8
LAG = 12
CUTS = (1 / 2,)
MESH = pl.DeviceIdType.MESH


def kernel(n, groups, q_hbm, k_hbm, v_hbm, out, q_ref, kb, vb, s0, s1, p0, p1, m0, m1, stats, parts, q_sem, k_sem, v_sem, last_sem, send, recv, stat_send, stat_recv):
    heads, head = q_ref.shape[1:]
    rows = kb.shape[1]
    half = rows // 2
    tiles = half // 128
    ends = [0, *(int(c * rows) for c in CUTS), rows]
    key_heads = groups[0]
    scale = head**-0.5 * math.log2(math.e)
    me = lax.axis_index("sp")
    size = parts.shape[0]
    s_bufs, p_bufs, m_bufs = (s0, s1), (p0, p1), (m0, m1)
    lane = lax.broadcasted_iota(jnp.int32, (heads, 128), 1)

    def peer(d):
        return {"sp": lax.rem(me + d, size)}

    def source(d):
        return lax.rem(me + size - d, size)

    def k_copy(i):
        slot = lax.rem(i, KEYS)
        return pltpu.make_async_copy(k_hbm.at[i], kb.at[slot], k_sem.at[slot])

    def v_copy(i):
        slot = lax.rem(i, VALUES)
        return pltpu.make_async_copy(v_hbm.at[i], vb.at[slot], v_sem.at[slot])

    def last_copy(c):
        slot, run = (n - 1) % VALUES, pl.ds(ends[c], ends[c + 1] - ends[c])
        return pltpu.make_async_copy(v_hbm.at[n - 1, run], vb.at[slot, run], last_sem.at[c])

    def part_copy(d, first, count, late, slot):
        ref = parts.at[slot, pl.ds(first, count)]
        return pltpu.make_async_remote_copy(ref, ref, send.at[d - 1], recv.at[d - 1, late], device_id=peer(d), device_id_type=MESH)

    def stat_copy(d, slot):
        return pltpu.make_async_remote_copy(stats.at[slot], stats.at[slot], stat_send.at[d - 1], stat_recv.at[d - 1], device_id=peer(d), device_id_type=MESH)

    def scores(i, u):
        q = q_ref[i]
        none = jnp.zeros_like(q)
        both = jnp.concatenate([jnp.concatenate([q, none], 1), jnp.concatenate([none, q], 1)], 0)
        slot = lax.rem(i, KEYS)
        keys = jnp.concatenate([kb[slot, :half], kb[slot, half:]], 1)
        s = lax.dot_general(both, keys, (((1,), (1,)), ((), ())), preferred_element_type=jnp.float32)
        s = jnp.where(jnp.tile(own, (1, tiles)), s, -jnp.inf)
        s_bufs[u][...] = s
        high = functools.reduce(jnp.maximum, [s[:, j * 128 : (j + 1) * 128] for j in range(tiles)])
        m_bufs[u][...] = jnp.maximum(high[:heads], high[heads:])

    def weights(i, u):
        high = jnp.max(m_bufs[u][...], 1, keepdims=True)
        w = jnp.exp2((s_bufs[u][...] - jnp.concatenate([high, high], 0)) * scale)
        p_bufs[u][lax.rem(lax.div(i, 2), LAG // 2)] = w.astype(jnp.bfloat16)
        total = functools.reduce(jnp.add, [w[:, j * 128 : (j + 1) * 128] for j in range(tiles)])
        total = jnp.sum(total[:heads] + total[heads:], 1, keepdims=True)
        stats[me, 0] = jnp.where(lane == i, high, stats[me, 0])
        stats[me, 1] = jnp.where(lane == i, total, stats[me, 1])

    def seen(i, u, begin, end):
        slot, h = lax.rem(i, VALUES), begin // half
        w = p_bufs[u].at[lax.rem(lax.div(i, 2), LAG // 2)]
        w = w[h * heads : (h + 1) * heads, begin - h * half : end - h * half]
        return jnp.dot(w, vb[slot, begin:end], preferred_element_type=jnp.float32)

    def seen_all(i, u):
        return seen(i, u, 0, half) + seen(i, u, half, rows)

    def keep(i, o):
        parts[me, i] = o.astype(jnp.bfloat16)

    def share(first, count, late):
        for d in sorted(range(1, size), key=lambda d: abs(2 * d - size)):
            part_copy(d, first, count, late, me).start()

    q_copy = pltpu.make_async_copy(q_hbm, q_ref, q_sem)
    q_copy.start()
    for i in range(KEYS):
        k_copy(i).start(priority=1)
    barrier = pltpu.get_barrier_semaphore()
    for d in range(1, size):
        pl.semaphore_signal(barrier, inc=1, device_id=peer(d), device_id_type=MESH)
    row = lax.broadcasted_iota(jnp.int32, (2 * heads, 128), 0)
    col = lax.broadcasted_iota(jnp.int32, (2 * heads, 128), 1)
    own = lax.rem(col, key_heads) == lax.div(lax.rem(row, heads), heads // key_heads)
    stats[me] = jnp.ones_like(stats[me])
    q_copy.wait()

    k_copy(0).wait()
    scores(0, 0)
    k_copy(1).wait()
    scores(1, 1)
    weights(0, 0)
    for i in range(2):
        k_copy(KEYS + i).start(priority=1)
    for i in range(VALUES - LAG + 2):
        v_copy(i).start(priority=1)

    def start_last():
        for c in range(len(CUTS) + 1):
            last_copy(c).start(priority=1)

    def next_values(i):
        @pl.when(i < n - 1)
        def _():
            v_copy(i).start(priority=1)

        @pl.when(i == n - 1)
        def _():
            start_last()

    def early(values, j, carry):
        for u in range(2):
            k_copy(2 * j + u).wait()
        for u in range(2):
            scores(2 * j + u, u)
            weights(2 * j + u - 1, 1 - u)
        for u in range(2):
            k_copy(2 * j + u + KEYS).start(priority=1)
            if values:
                v_copy(2 * j + u - LAG + VALUES).start(priority=1)
        return carry

    first = max(1, (LAG - VALUES) // 2)
    lax.fori_loop(1, first, functools.partial(early, False), 0)
    lax.fori_loop(first, LAG // 2, functools.partial(early, True), 0)
    pl.semaphore_wait(barrier, size - 1)

    def step(j, carry):
        for u in range(2):
            k_copy(2 * j + u).wait()
            v_copy(2 * j + u - LAG).wait()
        for u in range(2):
            t = 2 * j + u
            keep(t - LAG, seen_all(t - LAG, u))
            scores(t, u)
            weights(t - 1, 1 - u)
        share(2 * j - LAG, 2, 0)
        for u in range(2):
            t = 2 * j + u

            @pl.when(t + KEYS < n)
            def _():
                k_copy(t + KEYS).start(priority=1)

            next_values(t - LAG + VALUES)

        return carry

    lax.fori_loop(LAG // 2, n // 2, step, 0)
    weights(n - 1, 1)
    for d in range(1, size):
        stat_copy(d, me).start()

    def late(j, carry):
        for u in range(2):
            i = 2 * j + u
            v_copy(i).wait()
            keep(i, seen_all(i, u))
        share(2 * j, 2, 0)
        for u in range(2):
            next_values(2 * j + u + VALUES)
        return carry

    lax.fori_loop((n - LAG) // 2, n // 2 - 1, late, 0)
    v_copy(n - 2).wait()
    keep(n - 2, seen_all(n - 2, 0))
    share(n - 2, 1, 1)
    o = None
    for c in range(len(CUTS) + 1):
        last_copy(c).wait()
        x = seen(n - 1, 1, ends[c], ends[c + 1])
        o = x if o is None else o + x
    keep(n - 1, o)
    share(n - 1, 1, 1)

    for d in range(1, size):
        stat_copy(d, source(d)).wait_recv()
    highs = [stats[r, 0] for r in range(size)]
    high = functools.reduce(jnp.maximum, highs)
    factors = [jnp.exp2((h - high) * scale) for h in highs]
    total = functools.reduce(jnp.add, [f * stats[r, 1] for r, f in enumerate(factors)])
    factors = [f / total for f in factors]

    def together(i):
        terms = [parts[r, i].astype(jnp.float32) * f[:, i : i + 1] for r, f in enumerate(factors)]
        out[i] = functools.reduce(jnp.add, terms).astype(out.dtype)

    for d in range(1, size):
        part_copy(d, 0, n - 2, 0, source(d)).wait_recv()
    for i in range(n - 2):
        together(i)
    for d in range(1, size):
        part_copy(d, n - 2, 2, 1, source(d)).wait_recv()
    for x in range(2):
        together(n - 2 + x)
    for d in range(1, size):
        stat_copy(d, me).wait_send()
        part_copy(d, 0, n, 0, me).wait_send()


def solution(mesh):
    size = mesh.shape["sp"]

    def step(q, k, v):
        n, heads, head = q.shape
        tokens, key_heads = k.shape[1:3]
        rows = tokens * key_heads
        half = rows // 2
        f32 = jnp.float32
        dma = pltpu.SemaphoreType.DMA
        return pl.pallas_call(
            functools.partial(kernel, n, (key_heads,)),
            out_shape=pltpu.VMEM(q.shape, q.dtype),
            in_specs=[pl.BlockSpec(memory_space=pl.ANY)] * 3,
            out_specs=pl.BlockSpec(memory_space=pltpu.VMEM),
            scratch_shapes=[
                pltpu.VMEM(q.shape, q.dtype),
                pltpu.VMEM((KEYS, rows, head), k.dtype),
                pltpu.VMEM((VALUES, rows, head), v.dtype),
                *[pltpu.VMEM((2 * heads, half), f32)] * 2,
                *[pltpu.VMEM((LAG // 2, 2 * heads, half), jnp.bfloat16)] * 2,
                *[pltpu.VMEM((heads, 128), f32)] * 2,
                pltpu.VMEM((size, 2, heads, 128), f32),
                pltpu.VMEM((size, n, heads, head), jnp.bfloat16),
                dma,
                dma((KEYS,)),
                dma((VALUES,)),
                dma((len(CUTS) + 1,)),
                dma((size - 1,)),
                dma((size - 1, 2)),
                dma((size - 1,)),
                dma((size - 1,)),
            ],
            compiler_params=pltpu.CompilerParams(collective_id=0, has_side_effects=True, vmem_limit_bytes=60 * 2**20),
            name="attend",
        )(q, k.reshape(n, rows, head), v.reshape(n, rows, head))

    return jax.shard_map(
        step,
        mesh=mesh,
        in_specs=(P("dp", None, None), P("dp", "sp", None, None), P("dp", "sp", None, None)),
        out_specs=P("dp", None, None),
        check_vma=False,
    )
```

```python
import functools
import math

import jax
import jax.numpy as jnp
from jax import lax
from jax.experimental import pallas as pl
from jax.experimental.pallas import tpu as pltpu
from jax.sharding import PartitionSpec as P

KEYS = 8
VALUES = 8
LAG = 14
MESH = pl.DeviceIdType.MESH


def kernel(n, key_heads, q_hbm, k_hbm, v_hbm, out, q_ref, kb, vb, s0, s1, p0, p1, m0, m1, stats, parts, recv, stat_recv, q_sem, k_sem, v_sem, send, stat_send):
    heads, head = q_ref.shape[1:]
    rows = kb.shape[1]
    half = rows // 2
    tiles = half // 128
    scale = head**-0.5 * math.log2(math.e)
    me = lax.axis_index("sp")
    size = parts.shape[0]
    s_bufs, p_bufs, m_bufs = (s0, s1), (p0, p1), (m0, m1)
    lane = lax.broadcasted_iota(jnp.int32, (heads, 128), 1)

    def peer(d):
        return {"sp": lax.rem(me + d, size)}

    def source(d):
        return lax.rem(me + size - d, size)

    def k_copy(i):
        slot = lax.rem(i, KEYS)
        return pltpu.make_async_copy(k_hbm.at[i], kb.at[slot], k_sem.at[slot])

    def v_copy(i, h):
        slot, run = lax.rem(i, VALUES), pl.ds(h * half, half)
        return pltpu.make_async_copy(v_hbm.at[i, run], vb.at[slot, run], v_sem.at[slot, h])

    def part_copy(d, first, count, late, slot):
        ref = parts.at[slot, pl.ds(first, count)]
        return pltpu.make_async_remote_copy(ref, ref, send.at[d - 1], recv.at[d - 1, late], device_id=peer(d), device_id_type=MESH)

    def stat_copy(d, slot):
        return pltpu.make_async_remote_copy(stats.at[slot], stats.at[slot], stat_send.at[d - 1], stat_recv.at[d - 1], device_id=peer(d), device_id_type=MESH)

    def scores(i, u):
        q = q_ref[i]
        none = jnp.zeros_like(q)
        both = jnp.concatenate([jnp.concatenate([q, none], 1), jnp.concatenate([none, q], 1)], 0)
        slot = lax.rem(i, KEYS)
        keys = jnp.concatenate([kb[slot, :half], kb[slot, half:]], 1)
        s = lax.dot_general(both, keys, (((1,), (1,)), ((), ())), preferred_element_type=jnp.float32)
        s = jnp.where(jnp.tile(own, (1, tiles)), s, -jnp.inf)
        s_bufs[u][...] = s
        high = functools.reduce(jnp.maximum, [s[:, j * 128 : (j + 1) * 128] for j in range(tiles)])
        m_bufs[u][...] = jnp.maximum(high[:heads], high[heads:])

    def weights(i, u):
        high = jnp.max(m_bufs[u][...], 1, keepdims=True)
        w = jnp.exp2((s_bufs[u][...] - jnp.concatenate([high, high], 0)) * scale)
        p_bufs[u][lax.rem(lax.div(i, 2), LAG // 2)] = w.astype(jnp.bfloat16)
        total = functools.reduce(jnp.add, [w[:, j * 128 : (j + 1) * 128] for j in range(tiles)])
        total = jnp.sum(total[:heads] + total[heads:], 1, keepdims=True)
        stats[me, 0] = jnp.where(lane == i, high, stats[me, 0])
        stats[me, 1] = jnp.where(lane == i, total, stats[me, 1])

    def seen(i, u, h):
        w = p_bufs[u].at[lax.rem(lax.div(i, 2), LAG // 2)]
        values = vb[lax.rem(i, VALUES), h * half : (h + 1) * half]
        return jnp.dot(w[h * heads : (h + 1) * heads], values, preferred_element_type=jnp.float32)

    def keep(i, o):
        parts[me, i] = o.astype(jnp.bfloat16)

    def share(first, count, late):
        for d in sorted(range(1, size), key=lambda d: abs(2 * d - size)):
            part_copy(d, first, count, late, me).start()

    q_copy = pltpu.make_async_copy(q_hbm, q_ref, q_sem)
    q_copy.start()
    for i in range(KEYS):
        k_copy(i).start(priority=1)
    barrier = pltpu.get_barrier_semaphore()
    for d in range(1, size):
        pl.semaphore_signal(barrier, inc=1, device_id=peer(d), device_id_type=MESH)
    row = lax.broadcasted_iota(jnp.int32, (2 * heads, 128), 0)
    col = lax.broadcasted_iota(jnp.int32, (2 * heads, 128), 1)
    own = lax.rem(col, key_heads) == lax.div(lax.rem(row, heads), heads // key_heads)
    stats[me] = jnp.ones_like(stats[me])
    q_copy.wait()

    k_copy(0).wait()
    scores(0, 0)
    k_copy(1).wait()
    scores(1, 1)
    weights(0, 0)
    for i in range(2):
        k_copy(KEYS + i).start(priority=1)
    for i in range(VALUES - LAG + 2):
        start_values(i)

    def start_values(i):
        for h in range(2):
            v_copy(i, h).start(priority=1)

    def next_values(i):
        @pl.when(i < n)
        def _():
            start_values(i)

    def early(values, j, carry):
        for u in range(2):
            k_copy(2 * j + u).wait()
        for u in range(2):
            scores(2 * j + u, u)
            weights(2 * j + u - 1, 1 - u)
        for u in range(2):
            k_copy(2 * j + u + KEYS).start(priority=1)
            if values:
                start_values(2 * j + u - LAG + VALUES)
        return carry

    first = max(1, (LAG - VALUES) // 2)
    lax.fori_loop(1, first, functools.partial(early, False), 0)
    lax.fori_loop(first, LAG // 2, functools.partial(early, True), 0)
    pl.semaphore_wait(barrier, size - 1)

    def step(j, carry):
        for u in range(2):
            k_copy(2 * j + u).wait()
            for h in range(2):
                v_copy(2 * j + u - LAG, h).wait()
        for u in range(2):
            t = 2 * j + u
            keep(t - LAG, seen(t - LAG, u, 0) + seen(t - LAG, u, 1))
            scores(t, u)
            weights(t - 1, 1 - u)
        share(2 * j - LAG, 2, 0)
        for u in range(2):
            t = 2 * j + u

            @pl.when(t + KEYS < n)
            def _():
                k_copy(t + KEYS).start(priority=1)

            next_values(t - LAG + VALUES)

        return carry

    lax.fori_loop(LAG // 2, n // 2, step, 0)
    weights(n - 1, 1)
    for d in range(1, size):
        stat_copy(d, me).start()

    def late(j, carry):
        for u in range(2):
            i = 2 * j + u
            for h in range(2):
                v_copy(i, h).wait()
            keep(i, seen(i, u, 0) + seen(i, u, 1))
        share(2 * j, 2, 0)
        for u in range(2):
            next_values(2 * j + u + VALUES)
        return carry

    lax.fori_loop((n - LAG) // 2, n // 2 - 1, late, 0)
    for i in (n - 2, n - 1):
        o = None
        for h in range(2):
            v_copy(i, h).wait()
            x = seen(i, i % 2, h)
            o = x if o is None else o + x
        keep(i, o)
        share(i, 1, i // (n - 1))

    for d in range(1, size):
        stat_copy(d, source(d)).wait_recv()
    highs = [stats[r, 0] for r in range(size)]
    high = functools.reduce(jnp.maximum, highs)
    factors = [jnp.exp2((h - high) * scale) for h in highs]
    total = functools.reduce(jnp.add, [f * stats[r, 1] for r, f in enumerate(factors)])
    factors = [f / total for f in factors]

    def together(i):
        terms = [parts[r, i].astype(jnp.float32) * f[:, i : i + 1] for r, f in enumerate(factors)]
        out[i] = functools.reduce(jnp.add, terms).astype(out.dtype)

    for d in range(1, size):
        part_copy(d, 0, n - 1, 0, source(d)).wait_recv()
    for i in range(n - 1):
        together(i)
    for d in range(1, size):
        part_copy(d, n - 1, 1, 1, source(d)).wait_recv()
    together(n - 1)
    for d in range(1, size):
        stat_copy(d, me).wait_send()
        part_copy(d, 0, n, 0, me).wait_send()


def solution(mesh):
    size = mesh.shape["sp"]

    def step(q, k, v):
        n, heads, head = q.shape
        tokens, key_heads = k.shape[1:3]
        rows = tokens * key_heads
        half = rows // 2
        f32 = jnp.float32
        dma = pltpu.SemaphoreType.DMA

        def scoped(*refs):
            pl.run_scoped(
                functools.partial(kernel, n, key_heads, *refs),
                dma,
                dma((KEYS,)),
                dma((VALUES, 2)),
                dma((size - 1,)),
                dma((size - 1,)),
            )

        return pl.pallas_call(
            scoped,
            out_shape=pltpu.VMEM(q.shape, q.dtype),
            in_specs=[pl.BlockSpec(memory_space=pl.ANY)] * 3,
            out_specs=pl.BlockSpec(memory_space=pltpu.VMEM),
            scratch_shapes=[
                pltpu.VMEM(q.shape, q.dtype),
                pltpu.VMEM((KEYS, rows, head), k.dtype),
                pltpu.VMEM((VALUES, rows, head), v.dtype),
                *[pltpu.VMEM((2 * heads, half), f32)] * 2,
                *[pltpu.VMEM((LAG // 2, 2 * heads, half), jnp.bfloat16)] * 2,
                *[pltpu.VMEM((heads, 128), f32)] * 2,
                pltpu.VMEM((size, 2, heads, 128), f32),
                pltpu.VMEM((size, n, heads, head), jnp.bfloat16),
                dma((size - 1, 2)),
                dma((size - 1,)),
            ],
            compiler_params=pltpu.CompilerParams(collective_id=0, has_side_effects=True, vmem_limit_bytes=60 * 2**20),
            name="attend",
        )(q, k.reshape(n, rows, head), v.reshape(n, rows, head))

    return jax.shard_map(
        step,
        mesh=mesh,
        in_specs=(P("dp", None, None), P("dp", "sp", None, None), P("dp", "sp", None, None)),
        out_specs=P("dp", None, None),
        check_vma=False,
    )
```

```python
import functools
import math

import jax
import jax.numpy as jnp
from jax import lax
from jax.experimental import pallas as pl
from jax.experimental.pallas import tpu as pltpu
from jax.sharding import PartitionSpec as P

KEYS = 8
VALUES = 8
LAG = 14
MESH = pl.DeviceIdType.MESH


def kernel(n, key_heads, q_hbm, k_hbm, v_hbm, out, q_ref, kb, vb, s0, s1, p0, p1, m0, m1, stats, parts, recv, stat_recv, q_sem, k_sem, v_sem, send, stat_send):
    heads, head = q_ref.shape[1:]
    rows = kb.shape[1]
    half = rows // 2
    tiles = half // 128
    scale = head**-0.5 * math.log2(math.e)
    me = lax.axis_index("sp")
    size = parts.shape[0]
    s_bufs, p_bufs, m_bufs = (s0, s1), (p0, p1), (m0, m1)
    lane = lax.broadcasted_iota(jnp.int32, (heads, 128), 1)

    def peer(d):
        return {"sp": lax.rem(me + d, size)}

    def source(d):
        return lax.rem(me + size - d, size)

    def k_copy(i):
        slot = lax.rem(i, KEYS)
        return pltpu.make_async_copy(k_hbm.at[i], kb.at[slot], k_sem.at[slot])

    def v_copy(i, h):
        slot, run = lax.rem(i, VALUES), pl.ds(h * half, half)
        return pltpu.make_async_copy(v_hbm.at[i, run], vb.at[slot, run], v_sem.at[slot, h])

    def part_copy(d, first, count, late, slot):
        ref = parts.at[slot, pl.ds(first, count)]
        return pltpu.make_async_remote_copy(ref, ref, send.at[d - 1], recv.at[d - 1, late], device_id=peer(d), device_id_type=MESH)

    def stat_copy(d, slot):
        return pltpu.make_async_remote_copy(stats.at[slot], stats.at[slot], stat_send.at[d - 1], stat_recv.at[d - 1], device_id=peer(d), device_id_type=MESH)

    def scores(i, u):
        q = q_ref[i]
        none = jnp.zeros_like(q)
        both = jnp.concatenate([jnp.concatenate([q, none], 1), jnp.concatenate([none, q], 1)], 0)
        slot = lax.rem(i, KEYS)
        keys = jnp.concatenate([kb[slot, :half], kb[slot, half:]], 1)
        s = lax.dot_general(both, keys, (((1,), (1,)), ((), ())), preferred_element_type=jnp.float32)
        s = jnp.where(jnp.tile(own, (1, tiles)), s, -jnp.inf)
        s_bufs[u][...] = s
        high = functools.reduce(jnp.maximum, [s[:, j * 128 : (j + 1) * 128] for j in range(tiles)])
        m_bufs[u][...] = jnp.maximum(high[:heads], high[heads:])

    def weights(i, u):
        high = jnp.max(m_bufs[u][...], 1, keepdims=True)
        w = jnp.exp2((s_bufs[u][...] - jnp.concatenate([high, high], 0)) * scale)
        p_bufs[u][lax.rem(lax.div(i, 2), LAG // 2)] = w.astype(jnp.bfloat16)
        total = functools.reduce(jnp.add, [w[:, j * 128 : (j + 1) * 128] for j in range(tiles)])
        total = jnp.sum(total[:heads] + total[heads:], 1, keepdims=True)
        stats[me, 0] = jnp.where(lane == i, high, stats[me, 0])
        stats[me, 1] = jnp.where(lane == i, total, stats[me, 1])

    def seen(i, u, h):
        w = p_bufs[u].at[lax.rem(lax.div(i, 2), LAG // 2)]
        values = vb[lax.rem(i, VALUES), h * half : (h + 1) * half]
        return jnp.dot(w[h * heads : (h + 1) * heads], values, preferred_element_type=jnp.float32)

    def keep(i, o):
        parts[me, i] = o.astype(jnp.bfloat16)

    def share(first, count, late):
        for d in sorted(range(1, size), key=lambda d: abs(2 * d - size)):
            part_copy(d, first, count, late, me).start()

    q_copy = pltpu.make_async_copy(q_hbm, q_ref, q_sem)
    q_copy.start()
    for i in range(KEYS):
        k_copy(i).start(priority=1)
    barrier = pltpu.get_barrier_semaphore()
    for d in range(1, size):
        pl.semaphore_signal(barrier, inc=1, device_id=peer(d), device_id_type=MESH)
    row = lax.broadcasted_iota(jnp.int32, (2 * heads, 128), 0)
    col = lax.broadcasted_iota(jnp.int32, (2 * heads, 128), 1)
    own = lax.rem(col, key_heads) == lax.div(lax.rem(row, heads), heads // key_heads)
    stats[me] = jnp.ones_like(stats[me])
    q_copy.wait()

    k_copy(0).wait()
    scores(0, 0)
    k_copy(1).wait()
    scores(1, 1)
    weights(0, 0)
    for i in range(2):
        k_copy(KEYS + i).start(priority=1)
    for i in range(VALUES - LAG + 2):
        start_values(i)

    def start_values(i):
        for h in range(2):
            v_copy(i, h).start(priority=1)

    def next_values(i):
        @pl.when(i < n)
        def _():
            start_values(i)

    def early(values, j, carry):
        for u in range(2):
            k_copy(2 * j + u).wait()
        for u in range(2):
            scores(2 * j + u, u)
            weights(2 * j + u - 1, 1 - u)
        for u in range(2):
            k_copy(2 * j + u + KEYS).start(priority=1)
            if values:
                start_values(2 * j + u - LAG + VALUES)
        return carry

    first = max(1, (LAG - VALUES) // 2)
    lax.fori_loop(1, first, functools.partial(early, False), 0)
    lax.fori_loop(first, LAG // 2, functools.partial(early, True), 0)
    pl.semaphore_wait(barrier, size - 1)

    def step(j, carry):
        for u in range(2):
            k_copy(2 * j + u).wait()
            for h in range(2):
                v_copy(2 * j + u - LAG, h).wait()
        for u in range(2):
            t = 2 * j + u
            keep(t - LAG, seen(t - LAG, u, 0) + seen(t - LAG, u, 1))
            scores(t, u)
            weights(t - 1, 1 - u)
        share(2 * j - LAG, 2, 0)
        for u in range(2):
            t = 2 * j + u

            @pl.when(t + KEYS < n)
            def _():
                k_copy(t + KEYS).start(priority=1)

            next_values(t - LAG + VALUES)

        return carry

    lax.fori_loop(LAG // 2, n // 2, step, 0)
    weights(n - 1, 1)
    for d in range(1, size):
        stat_copy(d, me).start()

    def late(j, carry):
        for u in range(2):
            i = 2 * j + u
            for h in range(2):
                v_copy(i, h).wait()
            keep(i, seen(i, u, 0) + seen(i, u, 1))
        share(2 * j, 2, 0)
        for u in range(2):
            next_values(2 * j + u + VALUES)
        return carry

    lax.fori_loop((n - LAG) // 2, n // 2 - 1, late, 0)
    for i in (n - 2, n - 1):
        v_copy(i, 0).wait()
        if i == n - 1:
            m0[...] = seen(i, i % 2, 0)
            v_copy(i, 1).wait()
            o = m0[...] + seen(i, i % 2, 1)
        else:
            v_copy(i, 1).wait()
            o = seen(i, i % 2, 0) + seen(i, i % 2, 1)
        keep(i, o)
        share(i, 1, i // (n - 1))

    for d in range(1, size):
        stat_copy(d, source(d)).wait_recv()
    highs = [stats[r, 0] for r in range(size)]
    high = functools.reduce(jnp.maximum, highs)
    factors = [jnp.exp2((h - high) * scale) for h in highs]
    total = functools.reduce(jnp.add, [f * stats[r, 1] for r, f in enumerate(factors)])
    factors = [f / total for f in factors]

    def together(i):
        terms = [parts[r, i].astype(jnp.float32) * f[:, i : i + 1] for r, f in enumerate(factors)]
        out[i] = functools.reduce(jnp.add, terms).astype(out.dtype)

    for d in range(1, size):
        part_copy(d, 0, n - 1, 0, source(d)).wait_recv()
    for i in range(n - 1):
        together(i)
    for d in range(1, size):
        part_copy(d, n - 1, 1, 1, source(d)).wait_recv()
    together(n - 1)
    for d in range(1, size):
        stat_copy(d, me).wait_send()
        part_copy(d, 0, n, 0, me).wait_send()


def solution(mesh):
    size = mesh.shape["sp"]

    def step(q, k, v):
        n, heads, head = q.shape
        tokens, key_heads = k.shape[1:3]
        rows = tokens * key_heads
        half = rows // 2
        f32 = jnp.float32
        dma = pltpu.SemaphoreType.DMA

        def scoped(*refs):
            pl.run_scoped(
                functools.partial(kernel, n, key_heads, *refs),
                dma,
                dma((KEYS,)),
                dma((VALUES, 2)),
                dma((size - 1,)),
                dma((size - 1,)),
            )

        return pl.pallas_call(
            scoped,
            out_shape=pltpu.VMEM(q.shape, q.dtype),
            in_specs=[pl.BlockSpec(memory_space=pl.ANY)] * 3,
            out_specs=pl.BlockSpec(memory_space=pltpu.VMEM),
            scratch_shapes=[
                pltpu.VMEM(q.shape, q.dtype),
                pltpu.VMEM((KEYS, rows, head), k.dtype),
                pltpu.VMEM((VALUES, rows, head), v.dtype),
                *[pltpu.VMEM((2 * heads, half), f32)] * 2,
                *[pltpu.VMEM((LAG // 2, 2 * heads, half), jnp.bfloat16)] * 2,
                *[pltpu.VMEM((heads, 128), f32)] * 2,
                pltpu.VMEM((size, 2, heads, 128), f32),
                pltpu.VMEM((size, n, heads, head), jnp.bfloat16),
                dma((size - 1, 2)),
                dma((size - 1,)),
            ],
            compiler_params=pltpu.CompilerParams(collective_id=0, has_side_effects=True, vmem_limit_bytes=60 * 2**20),
            name="attend",
        )(q, k.reshape(n, rows, head), v.reshape(n, rows, head))

    return jax.shard_map(
        step,
        mesh=mesh,
        in_specs=(P("dp", None, None), P("dp", "sp", None, None), P("dp", "sp", None, None)),
        out_specs=P("dp", None, None),
        check_vma=False,
    )
```
